256 devices in a mesh: seq: 128 (over y, z_lo, x, core), par: 2 (over z_hi).
Axes of the slice: x: 4, y: 4, z: 8 (z_hi: 2, z_lo: 4; z = z_hi * 4 + z_lo), core: 2. Of those that a mesh axis runs over, the one named last changes fastest.
Arguments:
- states: float32 [32768, 128], P('seq'), may hold values from -6 to 6
- cotangent: float32 [32768, 128], P('seq'), may hold values from -6 to 6
- obs_count: int32 [256], P('seq'), may hold values from 16 to 128
- step_index: int32 [2, 32768], P(None, 'seq'), may hold values from 0 to 15
- step_table: float32 [16], replicated, may hold values from 0.05 to 0.25
- w_in: bfloat16 [128, 2048], P(None, 'par'), may hold values from -0.5 to 0.5
- b_hid: bfloat16 [2048], P('par'), may hold values from -3 to 3
- w_out: bfloat16 [128, 2048], P(None, 'par'), may hold values from -0.125 to 0.125
- b_out: float32 [128], replicated, may hold values from -3 to 3
Outputs:
- state_grad: float32 [32768, 128], P('seq')
- grad_in: float32 [128, 2048], P('seq', 'par')
- grad_out: float32 [128, 2048], P('seq', 'par')
The draws below stay inside these ranges and needn't reach their ends.
All inputs are finite; a program needn't handle non-finite values.
Results may differ from the reference program's by a relative error of at most 0.0055.
Values may be sent and summed in bfloat16 or wider, within the bound.
No kernel may reach another device: no remote copies, remote signals or barrier semaphores. Data moves between devices by JAX's collectives and lax.ppermute only.
A program may use at most 64 MiB of HBM per device.

```python
import math
import jax
import jax.numpy as jnp
from jax import lax

L = 128
H = 2048
SLOT = 128
SEQ_DEV = 2
NTAB = 16
SEQS = 256
ROWS = 32768


def plant(array, own_key, low, high):
    longest = array.shape.index(max(array.shape))
    spots = []
    for shift in (0, 1):
        where = [jax.random.randint(jax.random.fold_in(own_key, axis), (), 0, length) for axis, length in enumerate(array.shape)]
        where[longest] = (where[longest] + shift) % array.shape[longest]
        spots.append(tuple(where))
    return array.at[spots[0]].set(low).at[spots[1]].set(high)


def steps_of(stream_key, extent, cuts, smallest, high):
    loudness, own = 1.0, jax.random.fold_in(stream_key, 6)
    for dim, blocks in cuts:
        steps = jnp.exp(jax.random.uniform(jax.random.fold_in(own, dim), (blocks,), jnp.float32, smallest / len(cuts), high / len(cuts)))
        loudness = loudness * jnp.repeat(steps, extent[dim] // blocks).reshape([-1 if axis == dim else 1 for axis in range(len(extent))])
    return loudness


def scatter_about(own_key, dims, width, limit, cuts=(), kind=jnp.bfloat16):
    values = width * jax.random.normal(own_key, dims, jnp.float32)
    if cuts:
        values = values * steps_of(own_key, dims, cuts, -0.22, 0.18)
    return jnp.clip(values, -limit, limit).astype(kind)


def setup_inputs(seed: int = 0) -> dict:
    keys = jax.random.split(jax.random.key(seed), 10)
    return {
        "states": scatter_about(keys[0], (ROWS, L), 1.0, 6.0, ((0, 128),), jnp.float32),
        "cotangent": scatter_about(keys[1], (ROWS, L), 1.0, 6.0, ((0, 128),), jnp.float32),
        "obs_count": plant(jax.random.randint(keys[2], (SEQS,), SLOT // 8, SLOT + 1), jax.random.fold_in(keys[2], 1), SLOT // 8, SLOT).astype(jnp.int32),
        "step_index": plant(jax.random.randint(keys[3], (2, ROWS), 0, NTAB), jax.random.fold_in(keys[3], 1), 0, NTAB - 1).astype(jnp.int32),
        "step_table": jnp.clip(jnp.exp(jax.random.uniform(keys[4], (NTAB,), jnp.float32, math.log(0.05), math.log(0.25))), 0.05, 0.25),
        "w_in": scatter_about(keys[5], (L, H), L ** -0.5, 0.5, ((1, 2),)),
        "b_hid": scatter_about(keys[6], (H,), 0.5, 3.0, ((0, 2),)),
        "w_out": scatter_about(keys[7], (L, H), H ** -0.5, 0.125, ((1, 2),)),
        "b_out": scatter_about(keys[8], (L,), 0.5, 3.0, (), jnp.float32),
    }


COEF_A = [[], [1.0 / 5], [3.0 / 40, 9.0 / 40], [44.0 / 45, -56.0 / 15, 32.0 / 9], [19372.0 / 6561, -25360.0 / 2187, 64448.0 / 6561, -212.0 / 729], [9017.0 / 3168, -355.0 / 33, 46732.0 / 5247, 49.0 / 176, -5103.0 / 18656]]
COEF_B = [35.0 / 384, 0.0, 500.0 / 1113, 125.0 / 192, -2187.0 / 6784, 11.0 / 84]


def identity(value):
    return value


def field(state, w_in, b_hid, w_out, b_out, forward_sum):
    state_b = state.astype(jnp.bfloat16)
    hidden = jnp.tanh(jnp.dot(state_b, w_in, preferred_element_type=jnp.float32) + b_hid.astype(jnp.float32))
    hidden_b = hidden.astype(jnp.bfloat16)
    partial_out = jnp.einsum("rh,lh->rl", hidden_b, w_out, preferred_element_type=jnp.float32)
    return forward_sum(partial_out) + b_out, state_b, hidden, hidden_b


def sweep(states, initial, sizes_list, w_in, b_hid, w_out, b_out, forward_sum, backward_sum):
    value = states
    records = []
    for size_now in sizes_list:
        slopes = []
        saved = []
        for current in range(6):
            if current == 0:
                probe = value
            else:
                combo = COEF_A[current][0] * slopes[0]
                for previous in range(1, current):
                    combo = combo + COEF_A[current][previous] * slopes[previous]
                probe = value + size_now * combo
            slope, state_b, hidden, hidden_b = field(probe, w_in, b_hid, w_out, b_out, forward_sum)
            slopes.append(slope)
            saved.append((state_b, hidden, hidden_b))
        combo = COEF_B[0] * slopes[0]
        for current in range(2, 6):
            combo = combo + COEF_B[current] * slopes[current]
        value = value + size_now * combo
        records.append((size_now, saved))
    back = initial
    grad_in = jnp.zeros(w_in.shape, jnp.float32)
    grad_out = jnp.zeros(w_out.shape, jnp.float32)
    for size_now, saved in reversed(records):
        adjoints = [None] * 6
        total = back
        for current in reversed(range(6)):
            combo = COEF_B[current] * back
            for later in range(current + 1, 6):
                combo = combo + COEF_A[later][current] * adjoints[later]
            grad_b = (size_now * combo).astype(jnp.bfloat16)
            state_b, hidden, hidden_b = saved[current]
            inner = jnp.dot(grad_b, w_out, preferred_element_type=jnp.float32) * (1.0 - hidden * hidden)
            inner_b = inner.astype(jnp.bfloat16)
            partial_back = jnp.einsum("rh,lh->rl", inner_b, w_in, preferred_element_type=jnp.float32)
            adjoints[current] = backward_sum(partial_back)
            total = total + adjoints[current]
            grad_in = grad_in + jnp.einsum("rl,rh->lh", state_b, inner_b, preferred_element_type=jnp.float32)
            grad_out = grad_out + jnp.einsum("rl,rh->lh", grad_b, hidden_b, preferred_element_type=jnp.float32)
        back = total
    return back, grad_in, grad_out


def reference(states, cotangent, obs_count, step_index, step_table, w_in, b_hid, w_out, b_out):
    rows_all = states.shape[0]
    live = (jnp.arange(rows_all, dtype=jnp.int32) % SLOT) < jnp.repeat(obs_count, SLOT)
    initial = cotangent * live[:, None].astype(jnp.float32)
    first_size = step_table[step_index[0]][:, None]
    second_size = step_table[step_index[1]][:, None]
    block = SEQ_DEV * SLOT
    blocks = rows_all // block

    def one_block(carry, pieces):
        block_states, block_initial, size_first, size_second = pieces
        back, grad_in, grad_out = sweep(block_states, block_initial, (size_first, size_second), w_in, b_hid, w_out, b_out, identity, identity)
        return (carry[0] + grad_in, carry[1] + grad_out), back

    zeros = jnp.zeros(w_in.shape, jnp.float32)
    totals, backs = lax.scan(one_block, (zeros, zeros), (states.reshape(blocks, block, -1), initial.reshape(blocks, block, -1), first_size.reshape(blocks, block, 1), second_size.reshape(blocks, block, 1)))
    return backs.reshape(rows_all, -1), totals[0], totals[1]
```

```python
import jax
import jax.numpy as jnp
import numpy as np
from jax import lax
from jax.sharding import Mesh
from jax.sharding import PartitionSpec as P

SEQ = ("y", "z", "x", "core")
PLACE = SEQ + ("par",)
SIZES = (4, 4, 4, 2, 2)


def swapped(value, axis):
    at = PLACE.index(axis)
    pairs = []
    for source in range(int(np.prod(SIZES))):
        place = list(np.unravel_index(source, SIZES))
        place[at] = 1 - place[at]
        pairs.append((source, int(np.ravel_multi_index(place, SIZES))))
    return lax.ppermute(value, PLACE, pairs)

COEF_A = [
    [],
    [1.0 / 5],
    [3.0 / 40, 9.0 / 40],
    [44.0 / 45, -56.0 / 15, 32.0 / 9],
    [19372.0 / 6561, -25360.0 / 2187, 64448.0 / 6561, -212.0 / 729],
    [9017.0 / 3168, -355.0 / 33, 46732.0 / 5247, 49.0 / 176, -5103.0 / 18656],
]
COEF_B = [35.0 / 384, 0.0, 500.0 / 1113, 125.0 / 192, -2187.0 / 6784, 11.0 / 84]


def field(state, w_in, b_hid, w_out, b_out):
    state_b = state.astype(jnp.bfloat16)
    hidden = jnp.tanh(
        jnp.dot(state_b, w_in, preferred_element_type=jnp.float32) + b_hid.astype(jnp.float32)
    )
    hidden_b = hidden.astype(jnp.bfloat16)
    partial_out = jnp.einsum("rh,lh->rl", hidden_b, w_out, preferred_element_type=jnp.float32)
    return (partial_out + b_out, state_b, hidden, hidden_b)


def sweep(states, initial, sizes_list, w_in, b_hid, w_out, b_out, own):
    value = states
    records = []
    for size_now in sizes_list:
        slopes = []
        saved = []
        for current in range(6):
            if current == 0:
                probe = value
            else:
                combo = COEF_A[current][0] * slopes[0]
                for previous in range(1, current):
                    combo = combo + COEF_A[current][previous] * slopes[previous]
                probe = value + size_now * combo
            slope, state_b, hidden, hidden_b = field(probe, w_in, b_hid, w_out, b_out)
            slopes.append(slope)
            saved.append((state_b, hidden, hidden_b))
        combo = COEF_B[0] * slopes[0]
        for current in range(2, 6):
            combo = combo + COEF_B[current] * slopes[current]
        value = value + size_now * combo
        records.append((size_now, saved))
    back = initial
    grad_in = jnp.zeros((w_in.shape[0], own), jnp.float32)
    grad_out = jnp.zeros((w_in.shape[0], own), jnp.float32)
    for size_now, saved in reversed(records):
        adjoints = [None] * 6
        total = back
        for current in reversed(range(6)):
            combo = COEF_B[current] * back
            for later in range(current + 1, 6):
                combo = combo + COEF_A[later][current] * adjoints[later]
            grad_b = (size_now * combo).astype(jnp.bfloat16)
            state_b, hidden, hidden_b = saved[current]
            inner = jnp.dot(grad_b, w_out, preferred_element_type=jnp.float32) * (
                1.0 - hidden * hidden
            )
            inner_b = inner.astype(jnp.bfloat16)
            partial_back = jnp.einsum(
                "rh,lh->rl", inner_b, w_in, preferred_element_type=jnp.float32
            )
            adjoints[current] = partial_back
            total = total + adjoints[current]
            grad_in = grad_in + jnp.einsum(
                "rl,rh->lh", state_b, inner_b[:, :own], preferred_element_type=jnp.float32
            )
            grad_out = grad_out + jnp.einsum(
                "rl,rh->lh", grad_b, hidden_b[:, :own], preferred_element_type=jnp.float32
            )
        back = total
    return (back, grad_in, grad_out)


def per_device(states, cotangent, obs_count, step_index, step_table, w_in, b_hid, w_out, b_out):
    rows = states.shape[0]
    local_seqs = obs_count.shape[0]
    slot_count = rows // local_seqs
    live = (jnp.arange(slot_count, dtype=jnp.int32)[None, :] < obs_count[:, None]).reshape(rows)
    initial = cotangent * live[:, None].astype(jnp.float32)
    table_ids = jnp.arange(step_table.shape[0], dtype=jnp.int32)

    def lookup(indices):
        picked = jnp.where(indices[:, None] == table_ids[None, :], step_table[None, :], 0.0)
        return jnp.sum(picked, axis=1)[:, None]

    first_size = lookup(step_index[0])
    second_size = lookup(step_index[1])
    core = lax.axis_index("core")
    feats, own = w_in.shape
    mine = jnp.concatenate(
        [jnp.where(core == 0, w_in, w_out), jnp.broadcast_to(b_hid[None, :], (8, own))], axis=0
    )
    other = lax.all_gather(swapped(mine, "par"), "core")
    whole_in = jnp.concatenate([w_in, other[0, :feats]], axis=1)
    whole_out = jnp.concatenate([w_out, other[1, :feats]], axis=1)
    whole_bias = jnp.concatenate([b_hid, other[0, feats]])
    back, grad_in, grad_out = sweep(
        states, initial, (first_size, second_size), whole_in, whole_bias, whole_out, b_out, own
    )
    both = jnp.concatenate([grad_in, grad_out], axis=1).reshape(feats // 2, 2, 2 * own // 128, 128)
    keep = lax.dynamic_index_in_dim(both, core, 1, keepdims=False)
    send = lax.dynamic_index_in_dim(both, 1 - core, 1, keepdims=False)
    pair = (keep + swapped(send, "core")).astype(jnp.bfloat16)
    arrived = lax.all_to_all(pair, ("y", "z", "x"), split_axis=0, concat_axis=0, tiled=True)
    total = arrived.astype(jnp.float32).sum(axis=0).reshape(2, 1, own)
    return (back, total[0], total[1])


def solution(mesh):
    fine = Mesh(mesh.devices.reshape(SIZES), PLACE)
    return jax.shard_map(
        per_device,
        mesh=fine,
        in_specs=(
            P(SEQ, None),
            P(SEQ, None),
            P(SEQ),
            P(None, SEQ),
            P(),
            P(None, "par"),
            P("par"),
            P(None, "par"),
            P(),
        ),
        out_specs=(P(SEQ, None), P(SEQ, "par"), P(SEQ, "par")),
        check_vma=False,
    )
```

```python
import jax
import jax.numpy as jnp
import numpy as np
from jax import lax
from jax.experimental import pallas as pl
from jax.experimental.pallas import tpu as pltpu
from jax.sharding import Mesh
from jax.sharding import PartitionSpec as P

SEQ = ("y", "z", "x", "core")
PLACE = SEQ + ("par",)
SIZES = (4, 4, 4, 2, 2)


def swapped(value, axis):
    at = PLACE.index(axis)
    pairs = []
    for source in range(int(np.prod(SIZES))):
        place = list(np.unravel_index(source, SIZES))
        place[at] = 1 - place[at]
        pairs.append((source, int(np.ravel_multi_index(place, SIZES))))
    return lax.ppermute(value, PLACE, pairs)

COEF_A = [
    [],
    [1.0 / 5],
    [3.0 / 40, 9.0 / 40],
    [44.0 / 45, -56.0 / 15, 32.0 / 9],
    [19372.0 / 6561, -25360.0 / 2187, 64448.0 / 6561, -212.0 / 729],
    [9017.0 / 3168, -355.0 / 33, 46732.0 / 5247, 49.0 / 176, -5103.0 / 18656],
]
COEF_B = [35.0 / 384, 0.0, 500.0 / 1113, 125.0 / 192, -2187.0 / 6784, 11.0 / 84]
BLOCK = 256
F32, BF16 = jnp.float32, jnp.bfloat16


def dot(a, b, contract=(1, 0)):
    dims = (((contract[0],), (contract[1],)), ((), ()))
    return lax.dot_general(a, b, dims, preferred_element_type=F32)


def transposed(value):
    rows, columns = value.shape
    return jnp.concatenate(
        [
            jnp.concatenate([value[i : i + 128, j : j + 128].T for i in range(0, rows, 128)], axis=1)
            for j in range(0, columns, 128)
        ],
        axis=0,
    )


def sweep_kernel(
    core, states, initial, sizes, bias_out, in_own, out_own, bias_own, other,
    back, keep, send,
    in_t, out_t, hid, slope_of, probe, value, terms, acc_in, acc_out, square,
):
    feats, own = in_own.shape
    rows = states.shape[0]
    in_other, out_other, bias_other = other.at[0, :feats], other.at[1, :feats], other.at[0, feats:]
    for half, (w_in, w_out, bias) in enumerate(
        ((in_own, out_own, bias_own), (in_other, out_other, bias_other))
    ):
        for at in range(0, own, 128):
            to = pl.ds(half * own + at, 128)
            in_t[to, :feats] = w_in[:, at : at + 128].T
            low = jnp.concatenate(
                [bias[:, at : at + 128].astype(F32), jnp.zeros((128 - bias.shape[0], 128), F32)]
            )
            in_t[to, feats:] = low.T.astype(BF16)
            out_t[to, :] = w_out[:, at : at + 128].T
    value[...] = transposed(states[...])
    acc_in[...] = jnp.zeros_like(acc_in)
    acc_out[...] = jnp.zeros_like(acc_out)
    unit = jnp.where(lax.broadcasted_iota(jnp.int32, (feats, rows), 0) == 0, 1.0, 0.0).astype(BF16)
    bias_o = bias_out[...]

    def forward(step, _):
        size = sizes[step]
        for now in range(6):
            state = value[...]
            if now:
                combo = COEF_A[now][0] * terms[0]
                for before in range(1, now):
                    combo = combo + COEF_A[now][before] * terms[before]
                state = state + size * combo
            state_b = state.astype(BF16)
            probe[step, now] = state_b
            full = jnp.concatenate([state_b, unit], axis=0)
            for at in range(0, 2 * own, BLOCK):
                hidden = jnp.tanh(dot(in_t[at : at + BLOCK], full))
                hid[step, now, at : at + BLOCK] = hidden.astype(BF16)
                slope_of[step, now, at : at + BLOCK] = (1.0 - hidden * hidden).astype(BF16)
            terms[now] = (
                dot(out_own[...], hid[step, now, :own])
                + dot(out_other[...], hid[step, now, own:])
                + bias_o
            )
        combo = COEF_B[0] * terms[0]
        for now in range(2, 6):
            combo = combo + COEF_B[now] * terms[now]
        value[...] = value[...] + size * combo
        return 0

    lax.fori_loop(0, 2, forward, 0)
    value[...] = transposed(initial[...])

    def backward(turn, _):
        step = 1 - turn
        size = sizes[step]
        for now in reversed(range(6)):
            combo = COEF_B[now] * value[...]
            for later in range(now + 1, 6):
                combo = combo + COEF_A[later][now] * terms[later]
            grad_b = (size * combo).astype(BF16)
            for at in range(0, 2 * own, BLOCK):
                inner = dot(out_t[at : at + BLOCK], grad_b) * slope_of[
                    step, now, at : at + BLOCK
                ].astype(F32)
                slope_of[step, now, at : at + BLOCK] = inner.astype(BF16)
            terms[now] = dot(in_own[...], slope_of[step, now, :own]) + dot(
                in_other[...], slope_of[step, now, own:]
            )
            acc_in[...] += dot(slope_of[step, now, :own], probe[step, now], (1, 1))
            acc_out[...] += dot(hid[step, now, :own], grad_b, (1, 1))
        total = value[...]
        for now in reversed(range(6)):
            total = total + terms[now]
        value[...] = total
        return 0

    lax.fori_loop(0, 2, backward, 0)
    back[...] = transposed(value[...])
    tiles = own // 128
    for which, acc in enumerate((acc_in, acc_out)):
        for tile in range(tiles):
            at = which * tiles + tile
            square[at] = acc[tile * 128 : (tile + 1) * 128].T
    for side in range(2):

        @pl.when(core[0] == side)
        def _():
            for at in range(2 * tiles):
                line = pl.ds(at, feats // 2, stride=2 * tiles)
                keep[line, :] = square[at, pl.ds(side, feats // 2, stride=2), :]
                send[line, :] = square[at, pl.ds(1 - side, feats // 2, stride=2), :]


def run_sweep(core, states, initial, sizes, bias_out, in_own, out_own, bias_own, other):
    rows, feats = states.shape
    own = in_own.shape[1]
    lines = feats * own // 128
    space = pl.BlockSpec(memory_space=pltpu.VMEM)
    return pl.pallas_call(
        sweep_kernel,
        out_shape=(
            jax.ShapeDtypeStruct((rows, feats), F32),
            jax.ShapeDtypeStruct((lines, 128), F32),
            jax.ShapeDtypeStruct((lines, 128), F32),
        ),
        in_specs=[pl.BlockSpec(memory_space=pltpu.SMEM)] + [space] * 8,
        out_specs=(space,) * 3,
        scratch_shapes=[
            pltpu.VMEM((2 * own, 2 * feats), BF16),
            pltpu.VMEM((2 * own, feats), BF16),
            pltpu.VMEM((2, 6, 2 * own, rows), BF16),
            pltpu.VMEM((2, 6, 2 * own, rows), BF16),
            pltpu.VMEM((2, 6, feats, rows), BF16),
            pltpu.VMEM((feats, rows), F32),
            pltpu.VMEM((6, feats, rows), F32),
            pltpu.VMEM((own, feats), F32),
            pltpu.VMEM((own, feats), F32),
            pltpu.VMEM((own // 64, 128, 128), F32),
        ],
        compiler_params=pltpu.CompilerParams(vmem_limit_bytes=48 << 20),
        cost_estimate=pl.CostEstimate(
            flops=12 * 12 * rows * feats * own * 2, bytes_accessed=4 << 20, transcendentals=0
        ),
        name="sweep",
    )(core, states, initial, sizes, bias_out, in_own, out_own, bias_own, other)


def per_device(states, cotangent, obs_count, step_index, step_table, w_in, b_hid, w_out, b_out):
    rows = states.shape[0]
    local_seqs = obs_count.shape[0]
    slot_count = rows // local_seqs
    live = (jnp.arange(slot_count, dtype=jnp.int32)[None, :] < obs_count[:, None]).reshape(rows)
    initial = cotangent * live[:, None].astype(jnp.float32)
    table_ids = jnp.arange(step_table.shape[0], dtype=jnp.int32)

    def lookup(indices):
        picked = jnp.where(indices[:, None] == table_ids[None, :], step_table[None, :], 0.0)
        return jnp.sum(picked, axis=1)[None, :]

    sizes = jnp.stack([lookup(step_index[0]), lookup(step_index[1])])
    core = lax.axis_index("core")
    feats, own = w_in.shape
    bias = jnp.broadcast_to(b_hid[None, :], (8, own))
    mine = jnp.concatenate([jnp.where(core == 0, w_in, w_out), bias], axis=0)
    other = lax.all_gather(swapped(mine, "par"), "core")
    bias_out = jnp.broadcast_to(b_out[:, None], (feats, rows))
    back, keep, send = run_sweep(
        core.reshape(1), states, initial, sizes, bias_out, w_in, w_out, bias, other
    )
    keep, send = (v.reshape(feats // 2, 2 * own // 128, 128) for v in (keep, send))
    pair = (keep + swapped(send, "core")).astype(BF16)
    arrived = lax.all_to_all(pair, ("y", "z", "x"), split_axis=0, concat_axis=0, tiled=True)
    total = arrived.astype(F32).sum(axis=0).reshape(2, 1, own)
    return (back, total[0], total[1])


def solution(mesh):
    fine = Mesh(mesh.devices.reshape(SIZES), PLACE)
    return jax.shard_map(
        per_device,
        mesh=fine,
        in_specs=(
            P(SEQ, None),
            P(SEQ, None),
            P(SEQ),
            P(None, SEQ),
            P(),
            P(None, "par"),
            P("par"),
            P(None, "par"),
            P(),
        ),
        out_specs=(P(SEQ, None), P(SEQ, "par"), P(SEQ, "par")),
        check_vma=False,
    )
```

```python
import jax
import jax.numpy as jnp
import numpy as np
from jax import lax
from jax.experimental import pallas as pl
from jax.experimental.pallas import tpu as pltpu
from jax.sharding import Mesh
from jax.sharding import PartitionSpec as P

SEQ = ("y", "z", "x", "core")
PLACE = SEQ + ("par",)
SIZES = (4, 4, 4, 2, 2)


def swapped(value, axis):
    at = PLACE.index(axis)
    pairs = []
    for source in range(int(np.prod(SIZES))):
        place = list(np.unravel_index(source, SIZES))
        place[at] ^= 1
        pairs.append((source, int(np.ravel_multi_index(place, SIZES))))
    return lax.ppermute(value, PLACE, pairs)


COEF_A = [
    [],
    [1.0 / 5],
    [3.0 / 40, 9.0 / 40],
    [44.0 / 45, -56.0 / 15, 32.0 / 9],
    [19372.0 / 6561, -25360.0 / 2187, 64448.0 / 6561, -212.0 / 729],
    [9017.0 / 3168, -355.0 / 33, 46732.0 / 5247, 49.0 / 176, -5103.0 / 18656],
]
COEF_B = [35.0 / 384, 0.0, 500.0 / 1113, 125.0 / 192, -2187.0 / 6784, 11.0 / 84]
BLOCK = 256
F32, BF16 = jnp.float32, jnp.bfloat16


def dot(a, b, contract=(1, 0)):
    dims = (((contract[0],), (contract[1],)), ((), ()))
    return lax.dot_general(a, b, dims, preferred_element_type=F32)


def transposed(value):
    rows, columns = value.shape
    return jnp.concatenate(
        [
            jnp.concatenate([value[i : i + 128, j : j + 128].T for i in range(0, rows, 128)], axis=1)
            for j in range(0, columns, 128)
        ],
        axis=0,
    )


def turn_weights(w_in, w_out, bias, in_t, out_t, start):
    feats, units = w_in.shape
    for at in range(0, units, 128):
        to = pl.ds(start + at, 128)
        in_t[to, :feats] = w_in[:, at : at + 128].T
        low = jnp.concatenate(
            [bias[:, at : at + 128].astype(F32), jnp.zeros((128 - bias.shape[0], 128), F32)]
        )
        in_t[to, feats:] = low.T.astype(BF16)
        out_t[to, :] = w_out[:, at : at + 128].T


def prepare_kernel(states, initial, w_in, w_out, bias, states_t, initial_t, in_t, out_t):
    states_t[...] = transposed(states[...])
    initial_t[...] = transposed(initial[...])
    turn_weights(w_in, w_out, bias, in_t, out_t, 0)


def prepare(states, initial, w_in, w_out, bias):
    rows, feats = states.shape
    own = w_in.shape[1]
    space = pl.BlockSpec(memory_space=pltpu.VMEM)
    return pl.pallas_call(
        prepare_kernel,
        out_shape=(
            jax.ShapeDtypeStruct((feats, rows), F32),
            jax.ShapeDtypeStruct((feats, rows), F32),
            jax.ShapeDtypeStruct((own, 2 * feats), BF16),
            jax.ShapeDtypeStruct((own, feats), BF16),
        ),
        in_specs=[space] * 5,
        out_specs=(space,) * 4,
        compiler_params=pltpu.CompilerParams(vmem_limit_bytes=8 << 20),
        cost_estimate=pl.CostEstimate(flops=200_000_000, bytes_accessed=2 << 20, transcendentals=0),
        name="prepare",
    )(states, initial, w_in, w_out, bias)


def sweep_kernel(
    core, states_t, initial_t, in_t_own, out_t_own, sizes, bias_out, in_own, out_own, near, far,
    back, keep, send,
    in_t_other, out_t_other, hid, slope_of, probe, value, terms, acc_in, acc_out, square,
):
    feats, own = in_own.shape
    rows = states_t.shape[1]
    part = near.shape[2]
    for start, got in ((0, near), (part, far)):
        turn_weights(
            got.at[0, :feats], got.at[1, :feats], got.at[0, feats:], in_t_other, out_t_other, start
        )
    value[...] = states_t[...]
    acc_in[...] = jnp.zeros_like(acc_in)
    acc_out[...] = jnp.zeros_like(acc_out)
    unit = jnp.where(lax.broadcasted_iota(jnp.int32, (feats, rows), 0) == 0, 1.0, 0.0).astype(BF16)
    bias_o = bias_out[...]

    def rows_of(first, second, at):
        return first[at : at + BLOCK] if at < own else second[at - own : at - own + BLOCK]

    def forward(step, _):
        size = sizes[step]
        for now in range(6):
            state = value[...]
            if now:
                combo = COEF_A[now][0] * terms[0]
                for before in range(1, now):
                    combo = combo + COEF_A[now][before] * terms[before]
                state = state + size * combo
            state_b = state.astype(BF16)
            probe[step, now] = state_b
            full = jnp.concatenate([state_b, unit], axis=0)
            for at in range(0, 2 * own, BLOCK):
                hidden = jnp.tanh(dot(rows_of(in_t_own, in_t_other, at), full))
                hid[step, now, at : at + BLOCK] = hidden.astype(BF16)
                slope_of[step, now, at : at + BLOCK] = (1.0 - hidden * hidden).astype(BF16)
            terms[now] = (
                dot(out_own[...], hid[step, now, :own])
                + dot(near[1, :feats], hid[step, now, own : own + part])
                + dot(far[1, :feats], hid[step, now, own + part :])
                + bias_o
            )
        combo = COEF_B[0] * terms[0]
        for now in range(2, 6):
            combo = combo + COEF_B[now] * terms[now]
        value[...] = value[...] + size * combo
        return 0

    lax.fori_loop(0, 2, forward, 0)
    value[...] = initial_t[...]

    def backward(turn, _):
        step = 1 - turn
        size = sizes[step]
        for now in reversed(range(6)):
            combo = COEF_B[now] * value[...]
            for later in range(now + 1, 6):
                combo = combo + COEF_A[later][now] * terms[later]
            grad_b = (size * combo).astype(BF16)
            for at in range(0, 2 * own, BLOCK):
                inner = dot(rows_of(out_t_own, out_t_other, at), grad_b) * slope_of[
                    step, now, at : at + BLOCK
                ].astype(F32)
                slope_of[step, now, at : at + BLOCK] = inner.astype(BF16)
            terms[now] = (
                dot(in_own[...], slope_of[step, now, :own])
                + dot(near[0, :feats], slope_of[step, now, own : own + part])
                + dot(far[0, :feats], slope_of[step, now, own + part :])
            )
            acc_in[...] += dot(slope_of[step, now, :own], probe[step, now], (1, 1))
            acc_out[...] += dot(hid[step, now, :own], grad_b, (1, 1))
        total = value[...]
        for now in reversed(range(6)):
            total = total + terms[now]
        value[...] = total
        return 0

    lax.fori_loop(0, 2, backward, 0)
    back[...] = transposed(value[...])
    tiles = own // 128
    for which, acc in enumerate((acc_in, acc_out)):
        for tile in range(tiles):
            at = which * tiles + tile
            square[at] = acc[tile * 128 : (tile + 1) * 128].T
    for side in range(2):

        @pl.when(core[0] == side)
        def _():
            for at in range(2 * tiles):
                line = pl.ds(at, feats // 2, stride=2 * tiles)
                keep[line, :] = square[at, pl.ds(side, feats // 2, stride=2), :]
                send[line, :] = square[at, pl.ds(1 - side, feats // 2, stride=2), :]


def run_sweep(core, prepared, sizes, bias_out, in_own, out_own, near, far):
    feats, rows = prepared[0].shape
    own = in_own.shape[1]
    lines = feats * own // 128
    space = pl.BlockSpec(memory_space=pltpu.VMEM)
    return pl.pallas_call(
        sweep_kernel,
        out_shape=(
            jax.ShapeDtypeStruct((rows, feats), F32),
            jax.ShapeDtypeStruct((lines, 128), F32),
            jax.ShapeDtypeStruct((lines, 128), F32),
        ),
        in_specs=[pl.BlockSpec(memory_space=pltpu.SMEM)] + [space] * 10,
        out_specs=(space,) * 3,
        scratch_shapes=[
            pltpu.VMEM((own, 2 * feats), BF16),
            pltpu.VMEM((own, feats), BF16),
            pltpu.VMEM((2, 6, 2 * own, rows), BF16),
            pltpu.VMEM((2, 6, 2 * own, rows), BF16),
            pltpu.VMEM((2, 6, feats, rows), BF16),
            pltpu.VMEM((feats, rows), F32),
            pltpu.VMEM((6, feats, rows), F32),
            pltpu.VMEM((own, feats), F32),
            pltpu.VMEM((own, feats), F32),
            pltpu.VMEM((own // 64, 128, 128), F32),
        ],
        compiler_params=pltpu.CompilerParams(vmem_limit_bytes=48 << 20),
        cost_estimate=pl.CostEstimate(
            flops=12 * 12 * rows * feats * own * 2, bytes_accessed=4 << 20, transcendentals=0
        ),
        name="sweep",
    )(core, *prepared, sizes, bias_out, in_own, out_own, near, far)


def per_device(states, cotangent, obs_count, step_index, step_table, w_in, b_hid, w_out, b_out):
    rows = states.shape[0]
    local_seqs = obs_count.shape[0]
    slot_count = rows // local_seqs
    live = (jnp.arange(slot_count, dtype=jnp.int32)[None, :] < obs_count[:, None]).reshape(rows)
    initial = cotangent * live[:, None].astype(jnp.float32)
    table_ids = jnp.arange(step_table.shape[0], dtype=jnp.int32)

    def lookup(indices):
        picked = jnp.where(indices[:, None] == table_ids[None, :], step_table[None, :], 0.0)
        return jnp.sum(picked, axis=1)[None, :]

    sizes = jnp.stack([lookup(step_index[0]), lookup(step_index[1])])
    core = lax.axis_index("core")
    feats, own = w_in.shape
    part = own // 2
    bias = jnp.broadcast_to(b_hid[None, :], (8, own))
    odd = lax.axis_index("x") % 2
    layer = jnp.concatenate([jnp.where(core == 0, w_in, w_out), bias], axis=0)
    piece = jnp.where(odd == 0, layer[:, :part], layer[:, part:])
    near = swapped(piece, "par")
    far = swapped(near, "x")
    near, far = lax.all_gather(near, "core"), lax.all_gather(far, "core")
    bias_out = jnp.broadcast_to(b_out[:, None], (feats, rows))
    prepared = prepare(states, initial, w_in, w_out, bias)
    back, keep, send = run_sweep(
        core.reshape(1), prepared, sizes, bias_out, w_in, w_out, near, far
    )
    keep, send = (v.reshape(feats // 2, 2 * own // 128, 128) for v in (keep, send))
    pair = (keep + swapped(send, "core")).astype(BF16)
    arrived = lax.all_to_all(pair, ("y", "z", "x"), split_axis=0, concat_axis=0, tiled=True)
    total = arrived.astype(F32).sum(axis=0).reshape(2, 1, own)
    return (back, total[0], total[1])


def solution(mesh):
    fine = Mesh(mesh.devices.reshape(SIZES), PLACE)
    return jax.shard_map(
        per_device,
        mesh=fine,
        in_specs=(
            P(SEQ, None),
            P(SEQ, None),
            P(SEQ),
            P(None, SEQ),
            P(),
            P(None, "par"),
            P("par"),
            P(None, "par"),
            P(),
        ),
        out_specs=(P(SEQ, None), P(SEQ, "par"), P(SEQ, "par")),
        check_vma=False,
    )
```

```python
import functools

import jax
import jax.numpy as jnp
import numpy as np
from jax import lax
from jax.experimental import pallas as pl
from jax.experimental.pallas import tpu as pltpu
from jax.sharding import Mesh
from jax.sharding import PartitionSpec as P

SEQ = ("y", "z", "x", "core")
PLACE = SEQ + ("par",)
SIZES = (4, 4, 4, 2, 2)


def swapped(value, axis):
    at = PLACE.index(axis)
    pairs = []
    for source in range(int(np.prod(SIZES))):
        place = list(np.unravel_index(source, SIZES))
        place[at] ^= 1
        pairs.append((source, int(np.ravel_multi_index(place, SIZES))))
    return lax.ppermute(value, PLACE, pairs)


COEF_A = [
    [],
    [1.0 / 5],
    [3.0 / 40, 9.0 / 40],
    [44.0 / 45, -56.0 / 15, 32.0 / 9],
    [19372.0 / 6561, -25360.0 / 2187, 64448.0 / 6561, -212.0 / 729],
    [9017.0 / 3168, -355.0 / 33, 46732.0 / 5247, 49.0 / 176, -5103.0 / 18656],
]
COEF_B = [35.0 / 384, 0.0, 500.0 / 1113, 125.0 / 192, -2187.0 / 6784, 11.0 / 84]
F32, BF16 = jnp.float32, jnp.bfloat16
TILE, PIECE = 256, 128
PIECES = 8


def transposed(value):
    rows, columns = value.shape
    return jnp.concatenate(
        [
            jnp.concatenate([value[i : i + 128, j : j + 128].T for i in range(0, rows, 128)], axis=1)
            for j in range(0, columns, 128)
        ],
        axis=0,
    )


def turned_in(square, bias):
    low = jnp.concatenate([bias.astype(F32), jnp.zeros((128 - bias.shape[0], 128), F32)])
    return jnp.concatenate([square.T, low.T.astype(BF16)], axis=1)


def turned_out(square):
    return jnp.concatenate([square.T, jnp.zeros((128, 128), BF16)], axis=1)


def prepare_kernel(
    counts, table, states, cotangent, index, w_in, w_out, bias, b_out,
    states_t, initial_t, sizes, in_t, out_t, bias_t,
):
    rows = states.shape[0]
    states_t[...] = transposed(states[...])
    slot = lax.broadcasted_iota(jnp.int32, (1, rows), 1)
    slots = rows // counts.shape[0]
    live = jnp.zeros((1, rows), F32)
    for which in range(counts.shape[0]):
        first = which * slots
        inside = (slot >= first) & (slot < first + counts[which])
        live = jnp.where(inside, 1.0, live)
    initial_t[...] = transposed(cotangent[...]) * live
    size = jnp.zeros(index.shape, F32)
    for entry in range(table.shape[0]):
        size = jnp.where(index[...] == entry, table[entry], size)
    sizes[...] = size
    column = jnp.broadcast_to(b_out[...], (128, 128)).T
    bias_t[...] = jnp.concatenate([column, column], axis=1)
    for at in range(0, w_in.shape[1], 128):
        here = slice(at, at + 128)
        in_t[here] = turned_in(w_in[:, here], bias[:, here])
        out_t[here] = turned_out(w_out[:, here])


def prepare(counts, table, states, cotangent, index, w_in, w_out, bias, b_out):
    rows, feats = states.shape
    own = w_in.shape[1]
    space = pl.BlockSpec(memory_space=pltpu.VMEM)
    return pl.pallas_call(
        prepare_kernel,
        out_shape=(
            jax.ShapeDtypeStruct((feats, rows), F32),
            jax.ShapeDtypeStruct((feats, rows), F32),
            jax.ShapeDtypeStruct(index.shape, F32),
            jax.ShapeDtypeStruct((own, 2 * feats), BF16),
            jax.ShapeDtypeStruct((own, 2 * feats), BF16),
            jax.ShapeDtypeStruct((feats, rows), F32),
        ),
        in_specs=[pl.BlockSpec(memory_space=pltpu.SMEM)] * 2 + [space] * 7,
        out_specs=(space,) * 6,
        compiler_params=pltpu.CompilerParams(vmem_limit_bytes=8 << 20),
        cost_estimate=pl.CostEstimate(flops=200_000_000, bytes_accessed=2 << 20, transcendentals=0),
        name="prepare",
    )(counts, table, states, cotangent, index, w_in, w_out, bias, b_out)


def sweep_kernel(
    core, states_t, initial_t, sizes, in_t_own, out_t_own, bias_t, in_own, out_own,
    near, near_peer, far, far_peer,
    back, keep, send,
    in_t_other, out_t_other, in_other, out_other, hid, hid_own, inner_own, probe, value, terms, grads,
    *accumulators,
):
    feats, own = in_own.shape
    rows = states_t.shape[1]
    part = near.shape[1]
    tiles = 2 * own // TILE
    first_core = core[0] == 0
    for start, mine, peer in ((0, near, near_peer), (part, far, far_peer)):
        for at in range(0, part, 128):
            here, to = slice(at, at + 128), slice(start + at, start + at + 128)
            a, b = mine[:feats, here], peer[:feats, here]
            square_in, square_out = jnp.where(first_core, a, b), jnp.where(first_core, b, a)
            in_other[:, to] = square_in
            out_other[:, to] = square_out
            in_t_other[to] = turned_in(square_in, mine[feats:, here])
            out_t_other[to] = turned_out(square_out)
    grads[...] = jnp.zeros_like(grads)
    unit = jnp.where(lax.broadcasted_iota(jnp.int32, (feats, rows), 0) == 0, 1.0, 0.0).astype(BF16)
    nothing = jnp.zeros((feats, rows), BF16)
    held = [accumulators[:PIECES], accumulators[PIECES:]]
    turns = [0, 0]

    def push(q, tile, transpose=False):
        register = turns[q] % 2
        turns[q] += 1
        pltpu.matmul_push_rhs(tile, staging_register=register, mxu_index=q, transpose=transpose)
        return register

    def place(q, number):
        return (2 * number + q) * TILE

    def lines(first, second, at, count):
        return first[at : at + count] if at < own else second[at - own : at - own + count]

    def columns(first, second, at):
        return first[:, at : at + TILE] if at < own else second[:, at - own : at - own + TILE]

    def slot(q, piece):
        return held[q][piece % 7]

    def stream(weights, q, piece, register):
        at = place(q, piece // 2) + piece % 2 * PIECE
        pltpu.matmul_acc_lhs(
            slot(q, piece), lines(*weights, at, PIECE), load_staged_rhs=register
        )

    def forward(step, _):
        size = sizes[pl.ds(step, 1), :]
        for now in range(6):
            state = value[...]
            if now > 1:
                combo = COEF_A[now][0] * terms[0]
                for before in range(1, now - 1):
                    combo = combo + COEF_A[now][before] * terms[before]
                state = state + size * combo
            if now:
                state = state + (COEF_A[now][now - 1] * size) * terms[now - 1]
            state_b = state.astype(BF16)
            probe[step, now] = state_b
            full = jnp.concatenate([state_b, unit], axis=0)
            staged = [push(q, full) for q in range(2)]
            for piece in range(7):
                for q in range(2):
                    stream((in_t_own, in_t_other), q, piece, None if piece else staged[q])
            for number in range(4):
                ready = [[], []]
                for half in range(2):
                    for q in range(2):
                        piece = 2 * number + half
                        hidden = jnp.tanh(pltpu.matmul_pop(slot(q, piece)))
                        if piece == 0:
                            stream((in_t_own, in_t_other), q, 7, None)
                        hidden_b = hidden.astype(BF16)
                        at = place(q, number) + half * PIECE
                        hid[step, now, at : at + PIECE] = hidden
                        if number < 2:
                            hid_own[step, now, at : at + PIECE] = hidden_b
                        ready[q].append(hidden_b)
                for q in range(2):
                    register = push(q, jnp.concatenate(ready[q], axis=0))
                    pltpu.matmul_acc_lhs(
                        held[q][7],
                        columns(out_own, out_other, place(q, number)),
                        load_staged_rhs=register,
                    )
            terms[now] = pltpu.matmul_pop(held[0][7]) + pltpu.matmul_pop(held[1][7]) + bias_t[...]
        combo = COEF_B[0] * terms[0]
        for now in range(2, 6):
            combo = combo + COEF_B[now] * terms[now]
        value[...] = value[...] + size * combo
        return 0

    def collect(q, which, number):
        product = pltpu.matmul_pop(held[q][(1 if which else 3) + number])
        for half in range(2):
            at = which * (own // 128) + 2 * (2 * number + q) + half
            grads[at] += product[:, half * 128 : (half + 1) * 128]

    def backward(turn, _):
        step = 1 - turn
        size = sizes[pl.ds(step, 1), :]
        for now in reversed(range(6)):
            combo = COEF_B[now] * value[...]
            for later in range(5, now + 1, -1):
                combo = combo + COEF_A[later][now] * terms[later]
            combo = size * combo
            if now < 5:
                combo = combo + (COEF_A[now + 1][now] * size) * terms[now + 1]
            grad_b = combo.astype(BF16)
            full = jnp.concatenate([grad_b, nothing], axis=0)
            staged = [push(q, full) for q in range(2)]
            for piece in range(3):
                for q in range(2):
                    stream((out_t_own, out_t_other), q, piece, None if piece else staged[q])
            if now < 5:
                for number in range(2):
                    for q in range(2):
                        collect(q, 0, number)
            for piece in range(3, 7):
                for q in range(2):
                    stream((out_t_own, out_t_other), q, piece, None)
            late = []
            for number in range(2):
                for q in range(2):
                    at = place(q, number)
                    late.append(push(q, hid_own[step, now, at : at + TILE], transpose=True))
            for number in range(4):
                ready = [[], []]
                for half in range(2):
                    for q in range(2):
                        piece = 2 * number + half
                        at = place(q, number) + half * PIECE
                        hidden = hid[step, now, at : at + PIECE]
                        inner = pltpu.matmul_pop(slot(q, piece)) * (1.0 - hidden * hidden)
                        if piece == 0:
                            stream((out_t_own, out_t_other), q, 7, None)
                        inner_b = inner.astype(BF16)
                        if number < 2:
                            inner_own[at : at + PIECE] = inner_b
                        ready[q].append(inner_b)
                if number < 2:
                    for q in range(2):
                        pltpu.matmul_acc_lhs(
                            held[q][1 + number], grad_b, load_staged_rhs=late[2 * number + q]
                        )
                for q in range(2):
                    register = push(q, jnp.concatenate(ready[q], axis=0))
                    pltpu.matmul_acc_lhs(
                        held[q][7],
                        columns(in_own, in_other, place(q, number)),
                        load_staged_rhs=register,
                    )
            for number in range(2):
                for q in range(2):
                    at = place(q, number)
                    register = push(q, inner_own[at : at + TILE], transpose=True)
                    pltpu.matmul_acc_lhs(
                        held[q][3 + number], probe[step, now], load_staged_rhs=register
                    )
            for number in range(2):
                for q in range(2):
                    collect(q, 1, number)
            terms[now] = pltpu.matmul_pop(held[0][7]) + pltpu.matmul_pop(held[1][7])
        for number in range(2):
            for q in range(2):
                collect(q, 0, number)
        total = value[...]
        for now in reversed(range(6)):
            total = total + terms[now]
        value[...] = total
        return 0

    value[...] = states_t[...]
    lax.fori_loop(0, 2, forward, 0)
    value[...] = initial_t[...]
    lax.fori_loop(0, 2, backward, 0)
    back[...] = transposed(value[...])
    width = 2 * own // 128
    for side in range(2):

        @pl.when(core[0] == side)
        def _():
            for at in range(width):
                line = pl.ds(at, feats // 2, stride=width)
                keep[line, :] = grads[at, pl.ds(side, feats // 2, stride=2), :]
                send[line, :] = grads[at, pl.ds(1 - side, feats // 2, stride=2), :]


def scoped(count, *refs):
    specs = [pltpu.ACC(q)((PIECE, TILE), F32) for q in range(2) for _ in range(PIECES)]
    pl.run_scoped(lambda *accumulators: sweep_kernel(*refs, *accumulators), *specs)


def run_sweep(core, prepared, in_own, out_own, pieces):
    feats, rows = prepared[0].shape
    own = in_own.shape[1]
    lines = feats * own // 128
    space = pl.BlockSpec(memory_space=pltpu.VMEM)
    return pl.pallas_call(
        functools.partial(scoped, PIECES),
        out_shape=(
            jax.ShapeDtypeStruct((rows, feats), F32),
            jax.ShapeDtypeStruct((lines, 128), F32),
            jax.ShapeDtypeStruct((lines, 128), F32),
        ),
        in_specs=[pl.BlockSpec(memory_space=pltpu.SMEM)] + [space] * 12,
        out_specs=(space,) * 3,
        scratch_shapes=[
            pltpu.VMEM((own, 2 * feats), BF16),
            pltpu.VMEM((own, 2 * feats), BF16),
            pltpu.VMEM((feats, own), BF16),
            pltpu.VMEM((feats, own), BF16),
            pltpu.VMEM((2, 6, 2 * own, rows), F32),
            pltpu.VMEM((2, 6, own, rows), BF16),
            pltpu.VMEM((own, rows), BF16),
            pltpu.VMEM((2, 6, feats, rows), BF16),
            pltpu.VMEM((feats, rows), F32),
            pltpu.VMEM((6, feats, rows), F32),
            pltpu.VMEM((own // 64, feats, 128), F32),
        ],
        compiler_params=pltpu.CompilerParams(vmem_limit_bytes=38 << 20),
        cost_estimate=pl.CostEstimate(
            flops=12 * 12 * rows * feats * own * 2, bytes_accessed=4 << 20, transcendentals=0
        ),
        name="sweep",
    )(core, *prepared, in_own, out_own, *pieces)


def per_device(states, cotangent, obs_count, step_index, step_table, w_in, b_hid, w_out, b_out):
    core = lax.axis_index("core")
    feats, own = w_in.shape
    part = own // 2
    bias = jnp.broadcast_to(b_hid[None, :], (8, own))
    odd = lax.axis_index("x") % 2
    layer = jnp.concatenate([jnp.where(core == 0, w_in, w_out), bias], axis=0)
    piece = jnp.where(odd == 0, layer[:, :part], layer[:, part:])
    arrived = swapped(piece, "par")
    prepared = prepare(
        obs_count, step_table, states, cotangent, step_index, w_in, w_out, bias, b_out[None, :]
    )
    near, prepared = lax.optimization_barrier((arrived, prepared))
    far = swapped(near, "x")
    pieces = (near, swapped(near, "core"), far, swapped(far, "core"))
    back, keep, send = run_sweep(core.reshape(1), prepared, w_in, w_out, pieces)
    keep, send = (v.reshape(feats // 2, 2 * own // 128, 128) for v in (keep, send))
    pair = (keep + swapped(send, "core")).astype(BF16)
    arrived = lax.all_to_all(pair, ("y", "z", "x"), split_axis=0, concat_axis=0, tiled=True)
    total = arrived.astype(F32).sum(axis=0).reshape(2, 1, own)
    return (back, total[0], total[1])


def solution(mesh):
    fine = Mesh(mesh.devices.reshape(SIZES), PLACE)
    return jax.shard_map(
        per_device,
        mesh=fine,
        in_specs=(
            P(SEQ, None),
            P(SEQ, None),
            P(SEQ),
            P(None, SEQ),
            P(),
            P(None, "par"),
            P("par"),
            P(None, "par"),
            P(),
        ),
        out_specs=(P(SEQ, None), P(SEQ, "par"), P(SEQ, "par")),
        check_vma=False,
    )
```

```python
import functools

import jax
import jax.numpy as jnp
import numpy as np
from jax import lax
from jax.experimental import pallas as pl
from jax.experimental.pallas import tpu as pltpu
from jax.sharding import Mesh
from jax.sharding import PartitionSpec as P

SEQ = ("y", "z", "x", "core")
PLACE = SEQ + ("par",)
SIZES = (4, 4, 4, 2, 2)


def sent(value, other_place):
    pairs = []
    for source in range(int(np.prod(SIZES))):
        place = [int(v) for v in np.unravel_index(source, SIZES)]
        pairs.append((source, int(np.ravel_multi_index(other_place(*place), SIZES))))
    return lax.ppermute(value, PLACE, pairs)


def other_core(y, z, x, core, par):
    return y, z, x, 1 - core, par


def other_half(y, z, x, core, par):
    return y, SIZES[1] - 1 - z, x, core, 1 - par


COEF_A = [
    [],
    [1.0 / 5],
    [3.0 / 40, 9.0 / 40],
    [44.0 / 45, -56.0 / 15, 32.0 / 9],
    [19372.0 / 6561, -25360.0 / 2187, 64448.0 / 6561, -212.0 / 729],
    [9017.0 / 3168, -355.0 / 33, 46732.0 / 5247, 49.0 / 176, -5103.0 / 18656],
]
COEF_B = [35.0 / 384, 0.0, 500.0 / 1113, 125.0 / 192, -2187.0 / 6784, 11.0 / 84]
F32, BF16 = jnp.float32, jnp.bfloat16
TILE, PIECE = 256, 128
PIECES = 8


def transposed(value):
    rows, columns = value.shape
    return jnp.concatenate(
        [
            jnp.concatenate([value[i : i + 128, j : j + 128].T for i in range(0, rows, 128)], axis=1)
            for j in range(0, columns, 128)
        ],
        axis=0,
    )


def turned_in(square, bias):
    low = jnp.concatenate([bias.astype(F32), jnp.zeros((128 - bias.shape[0], 128), F32)])
    return jnp.concatenate([square.T, low.T.astype(BF16)], axis=1)


def prepare_kernel(
    counts, table, states, cotangent, index, w_in, w_out, layer, b_out,
    states_t, initial_t, sizes, in_t, out_t, bias_t,
):
    rows, feats = states.shape
    states_t[...] = transposed(states[...])
    slot = lax.broadcasted_iota(jnp.int32, (1, rows), 1)
    slots = rows // counts.shape[0]
    live = jnp.zeros((1, rows), F32)
    for which in range(counts.shape[0]):
        first = which * slots
        inside = (slot >= first) & (slot < first + counts[which])
        live = jnp.where(inside, 1.0, live)
    initial_t[...] = transposed(cotangent[...]) * live
    size = jnp.zeros(index.shape, F32)
    for entry in range(table.shape[0]):
        size = jnp.where(index[...] == entry, table[entry], size)
    sizes[...] = size
    column = jnp.broadcast_to(b_out[...], (128, 128)).T
    bias_t[...] = jnp.concatenate([column, column], axis=1)
    for at in range(0, w_in.shape[1], 128):
        here = slice(at, at + 128)
        in_t[here] = turned_in(w_in[:, here], layer[feats:, here])
        out_t[here] = w_out[:, here].T


def prepare(counts, table, states, cotangent, index, w_in, w_out, layer, b_out):
    rows, feats = states.shape
    own = w_in.shape[1]
    space = pl.BlockSpec(memory_space=pltpu.VMEM)
    return pl.pallas_call(
        prepare_kernel,
        out_shape=(
            jax.ShapeDtypeStruct((feats, rows), F32),
            jax.ShapeDtypeStruct((feats, rows), F32),
            jax.ShapeDtypeStruct(index.shape, F32),
            jax.ShapeDtypeStruct((own, 2 * feats), BF16),
            jax.ShapeDtypeStruct((own, feats), BF16),
            jax.ShapeDtypeStruct((feats, rows), F32),
        ),
        in_specs=[pl.BlockSpec(memory_space=pltpu.SMEM)] * 2 + [space] * 7,
        out_specs=(space,) * 6,
        compiler_params=pltpu.CompilerParams(vmem_limit_bytes=8 << 20),
        cost_estimate=pl.CostEstimate(flops=200_000_000, bytes_accessed=2 << 20, transcendentals=0),
        name="prepare",
    )(counts, table, states, cotangent, index, w_in, w_out, layer, b_out)


def sweep_kernel(
    core, states_t, initial_t, sizes, in_t_own, out_t_own, bias_t, in_own, out_own,
    near, near_peer,
    back, keep, send,
    in_t_other, out_t_other, in_other, out_other, hid, hid_own, inner_own, probe, value, terms, grads,
    *accumulators,
):
    feats, own = in_own.shape
    rows = states_t.shape[1]
    first_core = core[0] == 0
    for at in range(0, own, 128):
        here = slice(at, at + 128)
        a, b = near[:feats, here], near_peer[:feats, here]
        square_in, square_out = jnp.where(first_core, a, b), jnp.where(first_core, b, a)
        in_other[:, here] = square_in
        out_other[:, here] = square_out
        in_t_other[here] = turned_in(square_in, near[feats:, here])
        out_t_other[here] = square_out.T
    grads[...] = jnp.zeros_like(grads)
    unit = jnp.where(lax.broadcasted_iota(jnp.int32, (feats, rows), 0) == 0, 1.0, 0.0).astype(BF16)
    nothing = jnp.zeros((feats, rows), BF16)
    held = [accumulators[:PIECES], accumulators[PIECES:]]
    turns = [0, 0]

    def push(q, tile, transpose=False):
        register = turns[q] % 2
        turns[q] += 1
        pltpu.matmul_push_rhs(tile, staging_register=register, mxu_index=q, transpose=transpose)
        return register

    def place(q, number):
        return (2 * number + q) * TILE

    def lines(first, second, at, count):
        return first[at : at + count] if at < own else second[at - own : at - own + count]

    def columns(first, second, at):
        return first[:, at : at + TILE] if at < own else second[:, at - own : at - own + TILE]

    def slot(q, piece):
        return held[q][piece % 7]

    def stream(weights, q, piece, register):
        at = place(q, piece // 2) + piece % 2 * PIECE
        taken = lines(*weights, at, PIECE)
        if taken.shape[1] < TILE:
            taken = jnp.concatenate([taken, nothing[:, : TILE - taken.shape[1]]], axis=1)
        pltpu.matmul_acc_lhs(slot(q, piece), taken, load_staged_rhs=register)

    def forward(step, _):
        size = sizes[pl.ds(step, 1), :]
        for now in range(6):
            state = value[...]
            if now > 1:
                combo = COEF_A[now][0] * terms[0]
                for before in range(1, now - 1):
                    combo = combo + COEF_A[now][before] * terms[before]
                state = state + size * combo
            if now:
                state = state + (COEF_A[now][now - 1] * size) * terms[now - 1]
            state_b = state.astype(BF16)
            probe[step, now] = state_b
            full = jnp.concatenate([state_b, unit], axis=0)
            staged = [push(q, full) for q in range(2)]
            for piece in range(7):
                for q in range(2):
                    stream((in_t_own, in_t_other), q, piece, None if piece else staged[q])
            for number in range(4):
                ready = [[], []]
                for half in range(2):
                    for q in range(2):
                        piece = 2 * number + half
                        hidden = jnp.tanh(pltpu.matmul_pop(slot(q, piece)))
                        if piece == 0:
                            stream((in_t_own, in_t_other), q, 7, None)
                        hidden_b = hidden.astype(BF16)
                        at = place(q, number) + half * PIECE
                        hid[step, now, at : at + PIECE] = hidden
                        if number < 2:
                            hid_own[step, now, at : at + PIECE] = hidden_b
                        ready[q].append(hidden_b)
                for q in range(2):
                    register = push(q, jnp.concatenate(ready[q], axis=0))
                    pltpu.matmul_acc_lhs(
                        held[q][7],
                        columns(out_own, out_other, place(q, number)),
                        load_staged_rhs=register,
                    )
            terms[now] = pltpu.matmul_pop(held[0][7]) + pltpu.matmul_pop(held[1][7]) + bias_t[...]
        combo = COEF_B[0] * terms[0]
        for now in range(2, 6):
            combo = combo + COEF_B[now] * terms[now]
        value[...] = value[...] + size * combo
        return 0

    def collect(q, which, number):
        product = pltpu.matmul_pop(held[q][(1 if which else 3) + number])
        for half in range(2):
            at = which * (own // 128) + 2 * (2 * number + q) + half
            grads[at] += product[:, half * 128 : (half + 1) * 128]

    def backward(turn, _):
        step = 1 - turn
        size = sizes[pl.ds(step, 1), :]
        for now in reversed(range(6)):
            combo = COEF_B[now] * value[...]
            for later in range(5, now + 1, -1):
                combo = combo + COEF_A[later][now] * terms[later]
            combo = size * combo
            if now < 5:
                combo = combo + (COEF_A[now + 1][now] * size) * terms[now + 1]
            grad_b = combo.astype(BF16)
            full = jnp.concatenate([grad_b, nothing], axis=0)
            staged = [push(q, full) for q in range(2)]
            for piece in range(3):
                for q in range(2):
                    stream((out_t_own, out_t_other), q, piece, None if piece else staged[q])
            if now < 5:
                for number in range(2):
                    for q in range(2):
                        collect(q, 0, number)
            for piece in range(3, 7):
                for q in range(2):
                    stream((out_t_own, out_t_other), q, piece, None)
            late = []
            for number in range(2):
                for q in range(2):
                    at = place(q, number)
                    late.append(push(q, hid_own[step, now, at : at + TILE], transpose=True))
            for number in range(4):
                ready = [[], []]
                for half in range(2):
                    for q in range(2):
                        piece = 2 * number + half
                        at = place(q, number) + half * PIECE
                        hidden = hid[step, now, at : at + PIECE]
                        inner = pltpu.matmul_pop(slot(q, piece)) * (1.0 - hidden * hidden)
                        if piece == 0:
                            stream((out_t_own, out_t_other), q, 7, None)
                        inner_b = inner.astype(BF16)
                        if number < 2:
                            inner_own[at : at + PIECE] = inner_b
                        ready[q].append(inner_b)
                if number < 2:
                    for q in range(2):
                        pltpu.matmul_acc_lhs(
                            held[q][1 + number], grad_b, load_staged_rhs=late[2 * number + q]
                        )
                for q in range(2):
                    register = push(q, jnp.concatenate(ready[q], axis=0))
                    pltpu.matmul_acc_lhs(
                        held[q][7],
                        columns(in_own, in_other, place(q, number)),
                        load_staged_rhs=register,
                    )
            for number in range(2):
                for q in range(2):
                    at = place(q, number)
                    register = push(q, inner_own[at : at + TILE], transpose=True)
                    pltpu.matmul_acc_lhs(
                        held[q][3 + number], probe[step, now], load_staged_rhs=register
                    )
            for number in range(2):
                for q in range(2):
                    collect(q, 1, number)
            terms[now] = pltpu.matmul_pop(held[0][7]) + pltpu.matmul_pop(held[1][7])
        for number in range(2):
            for q in range(2):
                collect(q, 0, number)
        total = value[...]
        for now in reversed(range(6)):
            total = total + terms[now]
        value[...] = total
        return 0

    value[...] = states_t[...]
    lax.fori_loop(0, 2, forward, 0)
    value[...] = initial_t[...]
    lax.fori_loop(0, 2, backward, 0)
    back[...] = transposed(value[...])
    width = 2 * own // 128
    for side in range(2):

        @pl.when(core[0] == side)
        def _():
            for at in range(width):
                line = pl.ds(at, feats // 2, stride=width)
                keep[line, :] = grads[at, pl.ds(side, feats // 2, stride=2), :]
                send[line, :] = grads[at, pl.ds(1 - side, feats // 2, stride=2), :]


def scoped(count, *refs):
    specs = [pltpu.ACC(q)((PIECE, TILE), F32) for q in range(2) for _ in range(PIECES)]
    pl.run_scoped(lambda *accumulators: sweep_kernel(*refs, *accumulators), *specs)


def run_sweep(core, prepared, in_own, out_own, pieces):
    feats, rows = prepared[0].shape
    own = in_own.shape[1]
    lines = feats * own // 128
    space = pl.BlockSpec(memory_space=pltpu.VMEM)
    return pl.pallas_call(
        functools.partial(scoped, PIECES),
        out_shape=(
            jax.ShapeDtypeStruct((rows, feats), F32),
            jax.ShapeDtypeStruct((lines, 128), F32),
            jax.ShapeDtypeStruct((lines, 128), F32),
        ),
        in_specs=[pl.BlockSpec(memory_space=pltpu.SMEM)] + [space] * 10,
        out_specs=(space,) * 3,
        scratch_shapes=[
            pltpu.VMEM((own, 2 * feats), BF16),
            pltpu.VMEM((own, feats), BF16),
            pltpu.VMEM((feats, own), BF16),
            pltpu.VMEM((feats, own), BF16),
            pltpu.VMEM((2, 6, 2 * own, rows), F32),
            pltpu.VMEM((2, 6, own, rows), BF16),
            pltpu.VMEM((own, rows), BF16),
            pltpu.VMEM((2, 6, feats, rows), BF16),
            pltpu.VMEM((feats, rows), F32),
            pltpu.VMEM((6, feats, rows), F32),
            pltpu.VMEM((own // 64, feats, 128), F32),
        ],
        compiler_params=pltpu.CompilerParams(vmem_limit_bytes=38 << 20),
        cost_estimate=pl.CostEstimate(
            flops=12 * 12 * rows * feats * own * 2, bytes_accessed=4 << 20, transcendentals=0
        ),
        name="sweep",
    )(core, *prepared, in_own, out_own, *pieces)


def per_device(states, cotangent, obs_count, step_index, step_table, w_in, b_hid, w_out, b_out):
    core = lax.axis_index("core")
    feats, own = w_in.shape
    part = own // 2
    layer = jnp.concatenate(
        [jnp.where(core == 0, w_in, w_out), jnp.broadcast_to(b_hid[None, :], (8, own))], axis=0
    )
    arrived = sent(layer, other_half)
    prepared = prepare(
        obs_count, step_table, states, cotangent, step_index, w_in, w_out, layer, b_out[None, :]
    )
    near, prepared = lax.optimization_barrier((arrived, prepared))
    pieces = (near, sent(near, other_core))
    back, keep, send = run_sweep(core.reshape(1), prepared, w_in, w_out, pieces)
    keep, send = (v.reshape(feats // 2, 2 * own // 128, 128) for v in (keep, send))
    pair = (keep + sent(send, other_core)).astype(BF16)
    arrived = lax.all_to_all(pair, ("y", "z", "x"), split_axis=0, concat_axis=0, tiled=True)
    total = arrived.astype(F32).sum(axis=0).reshape(2, 1, own)
    return (back, total[0], total[1])


def solution(mesh):
    fine = Mesh(mesh.devices.reshape(SIZES), PLACE)
    return jax.shard_map(
        per_device,
        mesh=fine,
        in_specs=(
            P(SEQ, None),
            P(SEQ, None),
            P(SEQ),
            P(None, SEQ),
            P(),
            P(None, "par"),
            P("par"),
            P(None, "par"),
            P(),
        ),
        out_specs=(P(SEQ, None), P(SEQ, "par"), P(SEQ, "par")),
        check_vma=False,
    )
```
